128 devices in a mesh: rep: 1, dp: 128 (over x, y, z, core).
Axes of the slice: x: 4, y: 4, z: 4, core: 2. Of those that a mesh axis runs over, the one named last changes fastest.
Arguments:
- a: bfloat16 [128, 2, 4096, 1024], P(('rep', 'dp'))
- g: bfloat16 [128, 2, 4096, 3200], P(('rep', 'dp'))
Outputs:
- output: bfloat16 [2, 1024, 3200], P('rep')
All inputs are finite; a program needn't handle non-finite values.
Results may differ from the reference program's by a relative error of at most 0.012.
Values are sent between devices in bfloat16 or wider.
A program may use at most 1.5 GiB of HBM per device.

```python
import jax
import jax.numpy as jnp
from jax import lax

DEVICES = 128
MATRICES = 2
TOKENS = 4096
D = 1024
FF = 3200


def setup_inputs(seed: int = 0, part: int = 0) -> dict:
    ka, kg, ks = (jax.random.fold_in(k, part) for k in jax.random.split(jax.random.key(seed), 3))
    size = 2.0 ** jax.random.uniform(ks, (DEVICES, MATRICES, 1, 1), jnp.float32, -1.0, 1.0)
    a = jax.random.normal(ka, (DEVICES, MATRICES, TOKENS, D), jnp.float32)
    g = size * jax.random.normal(kg, (DEVICES, MATRICES, TOKENS, FF), jnp.float32) * (DEVICES * TOKENS) ** -0.5
    return {"a": a.astype(jnp.bfloat16), "g": g.astype(jnp.bfloat16)}


def reference(a, g):
    def take(so_far, one):
        term = jnp.einsum("ntd,ntf->ndf", *one, preferred_element_type=jnp.float32).astype(jnp.bfloat16)
        return so_far + term.astype(jnp.float32), None

    return lax.scan(take, jnp.zeros((MATRICES, D, FF), jnp.float32), (a, g))[0].astype(jnp.bfloat16)
```

```python
import jax
import jax.numpy as jnp
from jax import lax
from jax.experimental import pallas as pl
from jax.experimental.pallas import tpu as pltpu
from jax.sharding import PartitionSpec as P

BF, F32 = jnp.bfloat16, jnp.float32
MESH = pl.DeviceIdType.MESH
N, T, D, FF = 2, 4096, 1024, 3200
W = 256
PER = FF // W
NT = N * PER + 1
R = 8
LAG = (0, 1, 3, 5, 7, 9, 11, 13, 15, 17, 18)
CH = 512
NA = 4


def rows(start, size, unit):
    return pl.ds(pl.multiple_of(start, unit), size)


def kernel(a_ref, g_ref, out, raw, at, gb, acc, q2, q3, b0, b1a, b1b, b2, b3, r0, r1a, r1b, r2, r3,
           sem_a, sem_g, s0, s1a, s1b, s2, s3, t3, t2, t1a, t1b, t0, d0, d1a, d1b, d2, d3, e3, e2, e1a, e1b, e0):
    me = lax.axis_index("dp")
    c = lax.rem(me, 2)
    mate = me + 1 - 2 * c

    def ring(i, stage):
        axis = lax.rem(i + stage, 3)
        stride = jnp.where(axis == 0, 32, jnp.where(axis == 1, 8, 2))
        return stride, lax.rem(lax.div(me, stride), 4)

    def peer(r, d):
        stride, v = r
        return me + (lax.rem(v + d, 4) - v) * stride

    def send(src, dst, send_sem, recv_sem, to):
        return pltpu.make_async_remote_copy(src_ref=src, dst_ref=dst, send_sem=send_sem, recv_sem=recv_sem,
                                            device_id={"dp": to}, device_id_type=MESH)

    def block(i, h):
        last = i == NT - 1
        n = jnp.where(last, h, lax.div(i, PER))
        col = jnp.where(last, PER * W, lax.rem(i, PER) * W + h * 128)
        return n, pl.ds(pl.multiple_of(col, 128), 128)

    def c0(i):
        s = lax.rem(i, R)
        return [send(b0.at[s], r0.at[i], s0.at[s], d0.at[i], mate)]

    def c1a(i):
        s, r = lax.rem(i, R), ring(i, 0)
        return [send(b1a.at[s, k], r1a.at[i, k], s1a.at[s, k], d1a.at[i, k], peer(r, d)) for k, d in ((0, 1), (1, 3))]

    def c1b(i):
        s, r = lax.rem(i, R), ring(i, 0)
        return [send(b1b.at[s, k], r1b.at[i, k], s1b.at[s, k], d1b.at[i, k], peer(r, d)) for k, d in ((0, 1), (1, 3))]

    def c2(i):
        s, r = lax.rem(i, R), ring(i, 1)
        return [send(b2.at[s, k], r2.at[i, k], s2.at[s, k], d2.at[i, k], peer(r, k + 1)) for k in range(3)]

    def c3(i):
        s, r = lax.rem(i, R), ring(i, 2)
        return [send(b3.at[s, k], r3.at[i, k], s3.at[s, k], d3.at[i, k], peer(r, k + 1)) for k in range(3)]

    def part(i, start, size):
        n, cols = block(i, c)
        return out.at[n, rows(start, size, size), cols]

    def gather(i, start, size, r, d, ss, rs):
        return send(part(i, start, size), part(i, start, size), ss, rs, peer(r, d))

    def f3(i):
        s, x1, x2, x3 = lax.rem(i, R), ring(i, 0), ring(i, 1), ring(i, 2)
        return [gather(i, 256 * x1[1] + 64 * x2[1] + 16 * x3[1], 16, x3, k + 1, t3.at[s, k], e3.at[i, k]) for k in range(3)]

    def f2(i):
        s, x1, x2 = lax.rem(i, R), ring(i, 0), ring(i, 1)
        return [gather(i, 256 * x1[1] + 64 * x2[1], 64, x2, k + 1, t2.at[s, k], e2.at[i, k]) for k in range(3)]

    def f1a(i):
        s, x1 = lax.rem(i, R), ring(i, 0)
        return [gather(i, 256 * x1[1], 256, x1, d, t1a.at[s, k], e1a.at[i, k]) for k, d in ((0, 1), (1, 3))]

    def f1b(i):
        s, x1 = lax.rem(i, R), ring(i, 0)
        return [gather(i, 256 * lax.rem(x1[1] + 4 - d, 4) + 128 * k, 128, x1, d, t1b.at[s, k], e1b.at[i, k])
                for k, d in ((0, 1), (1, 3))]

    def f0(i, which):
        s, x1 = lax.rem(i, R), ring(i, 0)
        return [send(part(i, 256 * lax.rem(x1[1] + d, 4), 256), part(i, 256 * lax.rem(x1[1] + d, 4), 256), t0.at[s, k], e0.at[i, k], mate)
                for k, d in ((0, 0), (1, 3), (2, 1), (3, 2)) if k in which]

    def start(copies):
        for x in copies:
            x.start()

    def arrived(copies):
        for x in copies:
            x.wait_recv()

    def sent(copies):
        for x in copies:
            x.wait_send()

    def gcopies(i):
        s = lax.rem(i, 2)
        n, j = lax.div(i, PER), lax.rem(i, PER)
        return [pltpu.make_async_copy(g_ref.at[0, n, :, pl.ds(pl.multiple_of(j * W, 128), W)], gb.at[s], sem_g.at[s])]

    def glast():
        s = (NT - 1) % 2
        return [pltpu.make_async_copy(g_ref.at[0, n, :, pl.ds(PER * W, 128)], gb.at[s, :, pl.ds(128 * n, 128)], sem_g.at[2 * n])
                for n in range(N)]

    def acopy(i):
        s = lax.rem(i, NA)
        n, j = lax.div(i, T // CH), lax.rem(i, T // CH)
        return pltpu.make_async_copy(a_ref.at[0, n, rows(j * CH, CH, CH)], raw.at[s], sem_a.at[s])

    for k in range(NA - 1):
        acopy(k).start()
    start(gcopies(0))

    barrier = pltpu.get_barrier_semaphore()
    pl.semaphore_signal(barrier, inc=1, device_id={"dp": mate}, device_id_type=MESH)
    for axis in range(3):
        for d in (1, 2, 3):
            pl.semaphore_signal(barrier, inc=1, device_id={"dp": peer(ring(axis, 0), d)}, device_id_type=MESH)
    pl.semaphore_wait(barrier, 10)

    def transpose(i, carry):
        @pl.when(i + NA - 1 < N * T // CH)
        def _():
            acopy(i + NA - 1).start()

        acopy(i).wait()
        n, j = lax.div(i, T // CH), lax.rem(i, T // CH)
        at[n, :, pl.ds(pl.multiple_of(j * CH, CH), CH)] = raw[lax.rem(i, NA)].T
        return carry

    lax.fori_loop(0, N * T // CH, transpose, 0)

    def e_0(i):
        s = lax.rem(i, R)
        slot = lax.rem(i, 2)

        @pl.when(i < NT - 2)
        def _():
            start(gcopies(i + 1))

        @pl.when(i == NT - 2)
        def _():
            start(glast())

        @pl.when(i < NT - 1)
        def _():
            n = lax.div(i, PER)
            arrived_g = gcopies(i)
            arrived_g[0].wait()
            r = jnp.dot(at[n], gb[slot], preferred_element_type=F32)
            acc[s, 0] = r[:, :128]
            acc[s, 1] = r[:, 128:]

        @pl.when(i == NT - 1)
        def _():
            for x in glast():
                x.wait()
            for n in range(N):
                acc[s, n] = jnp.dot(at[n], gb[(NT - 1) % 2, :, 128 * n : 128 * n + 128], preferred_element_type=F32)

        b0[s] = acc[s, 1 - c].astype(BF)
        start(c0(i))

    def e_1(i):
        s, (_, v) = lax.rem(i, R), ring(i, 0)
        arrived(c0(i))
        acc[s, c] = acc[s, c] + r0[i].astype(F32)
        p = lax.rem(v + 2, 4) * 256
        for k in range(2):
            b1a[s, k] = acc[s, c, rows(p + 128 * k, 128, 128)].astype(BF)
        start(c1a(i))

    def e_2(i):
        s, (_, v) = lax.rem(i, R), ring(i, 0)
        sent(c0(i))
        arrived(c1a(i))
        for k, d in ((0, 1), (1, 3)):
            p = lax.rem(v + d, 4) * 256
            b1b[s, k, 128 * k : 128 * k + 128] = (acc[s, c, rows(p + 128 * k, 128, 128)] + r1a[i, k].astype(F32)).astype(BF)
            o = 1 - k
            b1b[s, k, 128 * o : 128 * o + 128] = acc[s, c, rows(p + 128 * o, 128, 128)].astype(BF)
        start(c1b(i))

    def e_3(i):
        s, (_, v), (_, w) = lax.rem(i, R), ring(i, 0), ring(i, 1)
        sent(c1a(i))
        arrived(c1b(i))
        q2[s] = acc[s, c, rows(v * 256, 256, 256)] + r1b[i, 0].astype(F32) + r1b[i, 1].astype(F32)
        for k in range(3):
            b2[s, k] = q2[s, rows(lax.rem(w + k + 1, 4) * 64, 64, 64)].astype(BF)
        start(c2(i))

    def e_4(i):
        s, (_, w), (_, u) = lax.rem(i, R), ring(i, 1), ring(i, 2)
        sent(c1b(i))
        arrived(c2(i))
        q3[s] = q2[s, rows(w * 64, 64, 64)] + r2[i, 0].astype(F32) + r2[i, 1].astype(F32) + r2[i, 2].astype(F32)
        for k in range(3):
            b3[s, k] = q3[s, rows(lax.rem(u + k + 1, 4) * 16, 16, 16)].astype(BF)
        start(c3(i))

    def e_5(i):
        s, (_, v), (_, w), (_, u) = lax.rem(i, R), ring(i, 0), ring(i, 1), ring(i, 2)
        sent(c2(i))
        arrived(c3(i))
        n, cols = block(i, c)
        total = q3[s, rows(u * 16, 16, 16)] + r3[i, 0].astype(F32) + r3[i, 1].astype(F32) + r3[i, 2].astype(F32)
        out[n, rows(256 * v + 64 * w + 16 * u, 16, 16), cols] = total.astype(BF)
        start(f3(i))

    def e_6(i):
        sent(c3(i))
        arrived(f3(i))
        start(f2(i))

    def e_7(i):
        sent(f3(i))
        arrived(f2(i))
        start(f1a(i))
        start(f0(i, (0,)))

    def e_8(i):
        sent(f2(i))
        arrived(f1a(i))
        start(f1b(i))
        start(f0(i, (1, 2)))

    def e_9(i):
        sent(f1a(i))
        arrived(f1b(i))
        start(f0(i, (3,)))

    def e_10(i):
        sent(f1b(i))
        for x in f0(i, (0, 1, 2, 3)):
            x.wait_send()
            x.wait_recv()

    steps = (e_0, e_1, e_2, e_3, e_4, e_5, e_6, e_7, e_8, e_9, e_10)

    def iteration(t, carry):
        for lag, step in zip(LAG, steps):
            i = t - lag

            @pl.when((i >= 0) & (i < NT))
            def _(i=i, step=step):
                step(i)

        return carry

    lax.fori_loop(0, NT + LAG[-1], iteration, 0)


def solution(mesh):
    dma = pltpu.SemaphoreType.DMA

    def step(a, g):
        return pl.pallas_call(
            kernel,
            out_shape=jax.ShapeDtypeStruct((N, D, FF), BF),
            in_specs=[pl.BlockSpec(memory_space=pl.ANY)] * 2,
            out_specs=pl.BlockSpec(memory_space=pltpu.VMEM),
            scratch_shapes=[
                pltpu.VMEM((NA, CH, D), BF), pltpu.VMEM((N, D, T), BF), pltpu.VMEM((2, T, W), BF),
                pltpu.VMEM((R, 2, D, 128), F32), pltpu.VMEM((R, 256, 128), F32), pltpu.VMEM((R, 64, 128), F32),
                pltpu.VMEM((R, D, 128), BF), pltpu.VMEM((R, 2, 128, 128), BF), pltpu.VMEM((R, 2, 256, 128), BF),
                pltpu.VMEM((R, 3, 64, 128), BF), pltpu.VMEM((R, 3, 16, 128), BF),
                pltpu.VMEM((NT, D, 128), BF), pltpu.VMEM((NT, 2, 128, 128), BF), pltpu.VMEM((NT, 2, 256, 128), BF),
                pltpu.VMEM((NT, 3, 64, 128), BF), pltpu.VMEM((NT, 3, 16, 128), BF),
                dma((NA,)), dma((3,)),
                dma((R,)), dma((R, 2)), dma((R, 2)), dma((R, 3)), dma((R, 3)),
                dma((R, 3)), dma((R, 3)), dma((R, 2)), dma((R, 2)), dma((R, 4)),
                dma((NT,)), dma((NT, 2)), dma((NT, 2)), dma((NT, 3)), dma((NT, 3)),
                dma((NT, 3)), dma((NT, 3)), dma((NT, 2)), dma((NT, 2)), dma((NT, 4)),
            ],
            compiler_params=pltpu.CompilerParams(collective_id=0, has_side_effects=True, vmem_limit_bytes=67043328),
        )(a, g)

    return jax.shard_map(step, mesh=mesh, in_specs=(P(("rep", "dp")), P(("rep", "dp"))), out_specs=P("rep"), check_vma=False)
```

```python
import jax
import jax.numpy as jnp
from jax import lax
from jax.experimental import pallas as pl
from jax.experimental.pallas import tpu as pltpu
from jax.sharding import PartitionSpec as P

BF, F32 = jnp.bfloat16, jnp.float32
MESH = pl.DeviceIdType.MESH
N, T, D, FF = 2, 4096, 1024, 3200
W = 256
PER = FF // W
NT = N * PER + 1
OWN = NT // 2 + 1
R = 4
LAG = (0, 1, 3, 5, 7, 9, 11, 13, 15, 16)
CH = 512
BLOCKS = T // CH
NA = 4


def rows(start, size, unit):
    return pl.ds(pl.multiple_of(start, unit), size)


def kernel(a_ref, g_ref, out, raw, at, gb, acc, q2, b0, b1a, b1b, b2, r0, r1a, r1b, r2, r3,
           sem_a, sem_g, s0, s1a, s1b, s2, s3, t2, t1a, t1b, t0, d0, d1a, d1b, d2, d3, e2, e1a, e1b, e0):
    me = lax.axis_index("dp")
    c = lax.rem(me, 2)
    mate = me + 1 - 2 * c

    def owner(i):
        return jnp.where(i >= NT - 2, 1, jnp.where(i == NT - 3, 0, 1 - lax.rem(i, 2)))

    def ring(i, stage):
        axis = lax.rem(i + stage, 3)
        stride = jnp.where(axis == 0, 32, jnp.where(axis == 1, 8, 2))
        return stride, lax.rem(lax.div(me, stride), 4)

    def peer(r, d):
        stride, v = r
        return me + (lax.rem(v + d, 4) - v) * stride

    def send(src, dst, send_sem, recv_sem, to):
        return pltpu.make_async_remote_copy(src_ref=src, dst_ref=dst, send_sem=send_sem, recv_sem=recv_sem,
                                            device_id={"dp": to}, device_id_type=MESH)

    def slots(i):
        j = lax.div(i, 2)
        return j, lax.rem(j, R)

    def c0(i):
        j, s = slots(i)
        return [send(b0.at[s], r0.at[j], s0.at[s], d0.at[j], mate)]

    def c1a(i):
        (j, s), r = slots(i), ring(i, 0)
        return [send(b1a.at[s, k], r1a.at[j, k], s1a.at[s, k], d1a.at[j, k], peer(r, d)) for k, d in ((0, 1), (1, 3))]

    def c1b(i):
        (j, s), r = slots(i), ring(i, 0)
        return [send(b1b.at[s, k], r1b.at[j, k], s1b.at[s, k], d1b.at[j, k], peer(r, d)) for k, d in ((0, 1), (1, 3))]

    def c2(i):
        (j, s), r = slots(i), ring(i, 1)
        return [send(b2.at[s, k], r2.at[j, k], s2.at[s, k], d2.at[j, k], peer(r, k + 1)) for k in range(3)]

    def c3(i):
        (j, s), r = slots(i), ring(i, 2)
        return [send(r3.at[j, r[1]], r3.at[j, r[1]], s3.at[s, k], d3.at[j, k], peer(r, k + 1)) for k in range(3)]

    def gather(i, start, size, to, ss, rs):
        piece = out.at[i, rows(start, size, size)]
        return send(piece, piece, ss, rs, to)

    def f2(i):
        (j, s), x1, x2 = slots(i), ring(i, 0), ring(i, 1)
        return [gather(i, 256 * x1[1] + 64 * x2[1], 64, peer(x2, k + 1), t2.at[s, k], e2.at[j, k]) for k in range(3)]

    def f1a(i):
        (j, s), x1 = slots(i), ring(i, 0)
        return [gather(i, 256 * x1[1], 256, peer(x1, d), t1a.at[s, k], e1a.at[j, k]) for k, d in ((0, 1), (1, 3))]

    def f1b(i):
        (j, s), x1 = slots(i), ring(i, 0)
        return [gather(i, 256 * lax.rem(x1[1] + 4 - d, 4) + 128 * k, 128, peer(x1, d), t1b.at[s, k], e1b.at[j, k])
                for k, d in ((0, 1), (1, 3))]

    def f0(i, which):
        (j, s), x1 = slots(i), ring(i, 0)
        return [gather(i, 256 * lax.rem(x1[1] + d, 4), 256, mate, t0.at[s, k], e0.at[i, k])
                for k, d in ((0, 0), (1, 3), (2, 1), (3, 2)) if k in which]

    def start(copies):
        for x in copies:
            x.start()

    def arrived(copies):
        for x in copies:
            x.wait_recv()

    def sent(copies):
        for x in copies:
            x.wait_send()

    def gcopy(i):
        s = lax.rem(i, 2)
        n, j = lax.div(i, PER), lax.rem(i, PER)
        return pltpu.make_async_copy(g_ref.at[0, n, :, pl.ds(pl.multiple_of(j * W, W), W)], gb.at[s], sem_g.at[s, 0])

    def glast():
        s = (NT - 1) % 2
        return [pltpu.make_async_copy(g_ref.at[0, n, :, pl.ds(PER * W, 128)], gb.at[s, :, pl.ds(128 * n, 128)], sem_g.at[s, n])
                for n in range(N)]

    def acopy(k):
        s = lax.rem(k, NA)
        n, j = lax.div(k, BLOCKS), lax.rem(k, BLOCKS)
        return pltpu.make_async_copy(a_ref.at[0, n, rows(j * CH, CH, CH)], raw.at[s], sem_a.at[s])

    barrier = pltpu.get_barrier_semaphore()
    pl.semaphore_signal(barrier, inc=1, device_id={"dp": mate}, device_id_type=MESH)
    for axis in range(3):
        for d in (1, 2, 3):
            pl.semaphore_signal(barrier, inc=1, device_id={"dp": peer(ring(axis, 0), d)}, device_id_type=MESH)

    for k in range(NA - 1):
        acopy(k).start()
    gcopy(0).start()

    def transpose(k):
        @pl.when(k + NA - 1 < N * BLOCKS)
        def _():
            acopy(k + NA - 1).start()

        acopy(k).wait()
        n, j = lax.div(k, BLOCKS), lax.rem(k, BLOCKS)
        at[n, :, rows(j * CH, CH, CH)] = raw[lax.rem(k, NA)].T

    def first(k, carry):
        transpose(k)
        return carry

    lax.fori_loop(0, BLOCKS, first, 0)
    pl.semaphore_wait(barrier, 10)

    def tile(i, mine):
        _, s = slots(i)
        slot = lax.rem(i, 2)

        @pl.when(i < NT - 1)
        def _():
            r = jnp.dot(at[lax.div(i, PER)], gb[slot], preferred_element_type=F32)
            if mine:
                acc[s] = r
            else:
                b0[s] = r.astype(BF)

        @pl.when(i == NT - 1)
        def _():
            for n in range(N):
                cols = slice(128 * n, 128 * n + 128)
                r = jnp.dot(at[n], gb[slot, :, cols], preferred_element_type=F32)
                if mine:
                    acc[s, :, cols] = r
                else:
                    b0[s, :, cols] = r.astype(BF)

    def e_0(i, mine):
        @pl.when(i < NT - 2)
        def _():
            gcopy(i + 1).start()

        @pl.when(i == NT - 2)
        def _():
            start(glast())

        @pl.when(i < NT - 1)
        def _():
            gcopy(i).wait()

        @pl.when(i == NT - 1)
        def _():
            for x in glast():
                x.wait()

        @pl.when(mine)
        def _():
            tile(i, True)

        @pl.when(jnp.logical_not(mine))
        def _():
            tile(i, False)
            start(c0(i))

        @pl.when(i < BLOCKS)
        def _():
            transpose(i + BLOCKS)

    def pair(i, at_row, size):
        j, s = slots(i)
        return acc[s, rows(at_row, size, size)] + r0[j, rows(at_row, size, size)].astype(F32)

    def e_1(i):
        (j, s), (_, v) = slots(i), ring(i, 0)
        arrived(c0(i))
        p = lax.rem(v + 2, 4) * 256
        for k in range(2):
            b1a[s, k] = pair(i, p + 128 * k, 128).astype(BF)
        start(c1a(i))

    def e_2(i):
        (j, s), (_, v) = slots(i), ring(i, 0)
        arrived(c1a(i))
        for k, d in ((0, 1), (1, 3)):
            p, o = lax.rem(v + d, 4) * 256, 1 - k
            b1b[s, k, 128 * k : 128 * k + 128] = (pair(i, p + 128 * k, 128) + r1a[j, k].astype(F32)).astype(BF)
            b1b[s, k, 128 * o : 128 * o + 128] = pair(i, p + 128 * o, 128).astype(BF)
        start(c1b(i))

    def e_3(i):
        (j, s), (_, v), (_, w) = slots(i), ring(i, 0), ring(i, 1)
        sent(c1a(i))
        arrived(c1b(i))
        q2[s] = pair(i, v * 256, 256) + r1b[j, 0].astype(F32) + r1b[j, 1].astype(F32)
        for k in range(3):
            b2[s, k] = q2[s, rows(lax.rem(w + k + 1, 4) * 64, 64, 64)].astype(BF)
        start(c2(i))

    def e_4(i):
        (j, s), (_, w), (_, u) = slots(i), ring(i, 1), ring(i, 2)
        sent(c1b(i))
        arrived(c2(i))
        partial = q2[s, rows(w * 64, 64, 64)] + r2[j, 0].astype(F32) + r2[j, 1].astype(F32) + r2[j, 2].astype(F32)
        r3[j, u] = partial.astype(BF)
        start(c3(i))

    def e_5(i):
        (j, s), (_, v), (_, w) = slots(i), ring(i, 0), ring(i, 1)
        sent(c2(i))
        arrived(c3(i))
        total = r3[j, 0].astype(F32) + r3[j, 1].astype(F32) + r3[j, 2].astype(F32) + r3[j, 3].astype(F32)
        out[i, rows(256 * v + 64 * w, 64, 64)] = total.astype(BF)
        start(f2(i))

    def e_6(i):
        sent(c3(i))
        arrived(f2(i))
        start(f1a(i))
        start(f0(i, (0,)))

    def e_7(i):
        sent(f2(i))
        arrived(f1a(i))
        start(f1b(i))
        start(f0(i, (1, 2)))

    def e_8(i):
        sent(f1a(i))
        arrived(f1b(i))
        start(f0(i, (3,)))

    def e_9(i):
        sent(f1b(i))
        sent(f0(i, (0, 1, 2, 3)))

    owned = (e_1, e_2, e_3, e_4, e_5, e_6, e_7, e_8, e_9)

    def iteration(t, carry):
        @pl.when(t < NT)
        def _():
            e_0(t, owner(t) == c)

        for lag, step in zip(LAG[1:], owned):
            i = t - lag
            inside = (i >= 0) & (i < NT)

            @pl.when(inside & (owner(i) == c))
            def _(i=i, step=step):
                step(i)

            if step is e_2 or step is e_9:
                @pl.when(inside & (owner(i) != c))
                def _(i=i, step=step):
                    if step is e_2:
                        sent(c0(i))
                    else:
                        arrived(f0(i, (0, 1, 2, 3)))

        return carry

    lax.fori_loop(0, NT + LAG[-1], iteration, 0)


def store(x, out, sems):
    copies = [pltpu.make_async_copy(x.at[i], out.at[i // PER, :, pl.ds(i % PER * W, W)], sems.at[i]) for i in range(NT - 1)]
    copies += [pltpu.make_async_copy(x.at[NT - 1, :, pl.ds(128 * n, 128)], out.at[n, :, pl.ds(PER * W, 128)], sems.at[NT - 1 + n])
               for n in range(N)]
    for y in copies:
        y.start()
    for y in copies:
        y.wait()


def solution(mesh):
    dma = pltpu.SemaphoreType.DMA

    def step(a, g):
        sums = pl.pallas_call(
            kernel,
            out_shape=pltpu.VMEM((NT, D, W), BF),
            in_specs=[pl.BlockSpec(memory_space=pl.ANY)] * 2,
            out_specs=pl.BlockSpec(memory_space=pltpu.VMEM),
            scratch_shapes=[
                pltpu.VMEM((NA, CH, D), BF), pltpu.VMEM((N, D, T), BF), pltpu.VMEM((2, T, W), BF),
                pltpu.VMEM((R, D, W), F32), pltpu.VMEM((R, 256, W), F32),
                pltpu.VMEM((R, D, W), BF), pltpu.VMEM((R, 2, 128, W), BF), pltpu.VMEM((R, 2, 256, W), BF),
                pltpu.VMEM((R, 3, 64, W), BF),
                pltpu.VMEM((OWN, D, W), BF), pltpu.VMEM((OWN, 2, 128, W), BF), pltpu.VMEM((OWN, 2, 256, W), BF),
                pltpu.VMEM((OWN, 3, 64, W), BF), pltpu.VMEM((OWN, 4, 64, W), BF),
                dma((NA,)), dma((2, 2)),
                dma((R,)), dma((R, 2)), dma((R, 2)), dma((R, 3)), dma((R, 3)),
                dma((R, 3)), dma((R, 2)), dma((R, 2)), dma((R, 4)),
                dma((OWN,)), dma((OWN, 2)), dma((OWN, 2)), dma((OWN, 3)), dma((OWN, 3)),
                dma((OWN, 3)), dma((OWN, 2)), dma((OWN, 2)), dma((NT, 4)),
            ],
            compiler_params=pltpu.CompilerParams(collective_id=0, has_side_effects=True, vmem_limit_bytes=50 * 1024 * 1024),
        )(a, g)
        return pl.pallas_call(
            store,
            out_shape=jax.ShapeDtypeStruct((N, D, FF), BF),
            in_specs=[pl.BlockSpec(memory_space=pltpu.VMEM)],
            out_specs=pl.BlockSpec(memory_space=pl.ANY),
            scratch_shapes=[dma((NT + 1,))],
            compiler_params=pltpu.CompilerParams(vmem_limit_bytes=1024 * 1024),
        )(sums)

    return jax.shard_map(step, mesh=mesh, in_specs=(P(("rep", "dp")), P(("rep", "dp"))), out_specs=P("rep"), check_vma=False)
```

```python
import jax
import jax.numpy as jnp
from jax import lax
from jax.experimental import pallas as pl
from jax.experimental.pallas import tpu as pltpu
from jax.sharding import PartitionSpec as P

BF, F32 = jnp.bfloat16, jnp.float32
MESH = pl.DeviceIdType.MESH
N, T, D, FF = 2, 4096, 1024, 3200
W = 256
PER = FF // W
WHOLE = N * PER
NT = WHOLE + N
OWN = NT // 2 + 1
R = 4
LAG = (0, 1, 3, 6, 8, 10, 13, 16, 18, 19)
HALF = (128, 128)
FROM = (0, HALF[0])
CH = 512
BLOCKS = T // CH
NA = 4


def rows(start, size, unit):
    return pl.ds(pl.multiple_of(start, unit), size)


def kernel(a_ref, g_ref, out, raw, at, gb, acc, q2, b0, b1a, b1b, b2, r0, r1a, r1b, r2, r3,
           sem_a, sem_g, s0, s1a, s1b, s2, s3, t2, t1a, t1b, t0, d0, d1a, d1b, d2, d3, e2, e1a, e1b, e0):
    me = lax.axis_index("dp")
    c = lax.rem(me, 2)
    mate = me + 1 - 2 * c

    def owner(i):
        return jnp.where(i >= NT - 3, 1, jnp.where(i == NT - 4, 0, 1 - lax.rem(i, 2)))

    place = (lax.div(me, 32), lax.rem(lax.div(me, 8), 4), lax.rem(lax.div(me, 2), 4))

    def ring(i, stage):
        axis = lax.rem(i + stage, 3)
        return jnp.where(axis == 0, 32, jnp.where(axis == 1, 8, 2)), jnp.where(axis == 0, place[0], jnp.where(axis == 1, place[1], place[2]))

    def peer(r, d):
        stride, v = r
        return me + (lax.rem(v + d, 4) - v) * stride

    def send(src, dst, send_sem, recv_sem, to):
        return pltpu.make_async_remote_copy(src_ref=src, dst_ref=dst, send_sem=send_sem, recv_sem=recv_sem,
                                            device_id={"dp": to}, device_id_type=MESH)

    def slots(i):
        j = jnp.where(i == NT - 1, OWN - 1, lax.div(i, 2))
        return j, lax.rem(j, R)

    def c0(i, w):
        j, s = slots(i)
        return [send(b0.at[s, :, pl.ds(0, w)], r0.at[j, :, pl.ds(0, w)], s0.at[s], d0.at[j], mate)]

    def c1a(i, w):
        (j, s), r = slots(i), ring(i, 0)
        return [send(b1a.at[s, pl.ds(FROM[k], HALF[k]), pl.ds(0, w)], r1a.at[j, pl.ds(FROM[k], HALF[k]), pl.ds(0, w)], s1a.at[s, k], d1a.at[j, k], peer(r, d))
                for k, d in ((0, 1), (1, 3))]

    def c1b(i, w):
        (j, s), r = slots(i), ring(i, 0)
        return [send(b1b.at[s, k, :, pl.ds(0, w)], r1b.at[j, k, :, pl.ds(0, w)], s1b.at[s, k], d1b.at[j, k], peer(r, d)) for k, d in ((0, 1), (1, 3))]

    def c2(i, w):
        (j, s), r = slots(i), ring(i, 1)
        return [send(b2.at[s, k, :, pl.ds(0, w)], r2.at[j, k, :, pl.ds(0, w)], s2.at[s, k], d2.at[j, k], peer(r, k + 1)) for k in range(3)]

    def c3(i, w):
        (j, s), r = slots(i), ring(i, 2)
        return [send(r3.at[j, r[1], :, pl.ds(0, w)], r3.at[j, r[1], :, pl.ds(0, w)], s3.at[s, k], d3.at[j, k], peer(r, k + 1)) for k in range(3)]

    def sums(i, start, size, w):
        if w == W:
            return i, rows(start, size, 32), pl.ds(0, W)
        return WHOLE, rows(start, size, 32), pl.ds(pl.multiple_of(128 * (i - WHOLE), 128), w)

    def gather(i, w, start, size, to, ss, rs):
        piece = out.at[sums(i, start, size, w)]
        return send(piece, piece, ss, rs, to)

    def f2(i, w):
        (j, s), x1, x2 = slots(i), ring(i, 0), ring(i, 1)
        return [gather(i, w, 256 * x1[1] + 64 * x2[1], 64, peer(x2, k + 1), t2.at[s, k], e2.at[j, k]) for k in range(3)]

    def f1a(i, w):
        (j, s), x1 = slots(i), ring(i, 0)
        return [gather(i, w, 256 * x1[1], 256, peer(x1, d), t1a.at[s, k], e1a.at[j, k]) for k, d in ((0, 1), (1, 3))]

    def f1b(i, w):
        (j, s), x1 = slots(i), ring(i, 0)
        return [gather(i, w, 256 * lax.rem(x1[1] + 4 - d, 4) + FROM[k], HALF[k], peer(x1, d), t1b.at[s, k], e1b.at[j, k])
                for k, d in ((0, 1), (1, 3))]

    def f0(i, w, which):
        (j, s), x1 = slots(i), ring(i, 0)
        return [gather(i, w, 256 * lax.rem(x1[1] + d, 4), 256, mate, t0.at[s, k], e0.at[i, k])
                for k, d in ((0, 0), (1, 3), (2, 1), (3, 2)) if k in which]

    def start(copies):
        for x in copies:
            x.start()

    def arrived(copies):
        for x in copies:
            x.wait_recv()

    def sent(copies):
        for x in copies:
            x.wait_send()

    def gcopy(i):
        s = lax.rem(i, 2)
        n, j = lax.div(i, PER), lax.rem(i, PER)
        return pltpu.make_async_copy(g_ref.at[0, n, :, pl.ds(pl.multiple_of(j * W, W), W)], gb.at[s], sem_g.at[s])

    def gnarrow(i):
        s = lax.rem(i, 2)
        return pltpu.make_async_copy(g_ref.at[0, i - WHOLE, :, pl.ds(PER * W, 128)], gb.at[s, :, pl.ds(0, 128)], sem_g.at[s])

    def acopy(k):
        s = lax.rem(k, NA)
        n, j = lax.div(k, BLOCKS), lax.rem(k, BLOCKS)
        return pltpu.make_async_copy(a_ref.at[0, n, rows(j * CH, CH, CH)], raw.at[s], sem_a.at[s])

    barrier = pltpu.get_barrier_semaphore()
    pl.semaphore_signal(barrier, inc=1, device_id={"dp": mate}, device_id_type=MESH)
    for axis in range(3):
        for d in (1, 2, 3):
            pl.semaphore_signal(barrier, inc=1, device_id={"dp": peer(ring(axis, 0), d)}, device_id_type=MESH)

    for k in range(NA - 1):
        acopy(k).start()
    gcopy(0).start()

    def transpose(k):
        @pl.when(k + NA - 1 < N * BLOCKS)
        def _():
            acopy(k + NA - 1).start()

        acopy(k).wait()
        n, j = lax.div(k, BLOCKS), lax.rem(k, BLOCKS)
        at[n, :, rows(j * CH, CH, CH)] = raw[lax.rem(k, NA)].T

    def first(k, carry):
        transpose(k)
        return carry

    lax.fori_loop(0, BLOCKS, first, 0)
    pl.semaphore_wait(barrier, 10)

    def tile(i, w, mine):
        _, s = slots(i)
        r = jnp.dot(at[lax.div(i, PER) if w == W else i - WHOLE], gb[lax.rem(i, 2), :, :w], preferred_element_type=F32)
        if mine:
            acc[s, :, :w] = r
        else:
            b0[s, :, :w] = r.astype(BF)
            start(c0(i, w))

    def e_0(i, mine):
        @pl.when(i + 1 < WHOLE)
        def _():
            gcopy(i + 1).start()

        @pl.when((i + 1 >= WHOLE) & (i + 1 < NT))
        def _():
            gnarrow(i + 1).start()

        @pl.when(i < WHOLE)
        def _():
            gcopy(i).wait()

        @pl.when(i >= WHOLE)
        def _():
            gnarrow(i).wait()

        for w, fits in ((W, i < WHOLE), (128, i >= WHOLE)):
            @pl.when(fits & mine)
            def _(w=w):
                tile(i, w, True)

            @pl.when(fits & jnp.logical_not(mine))
            def _(w=w):
                tile(i, w, False)

        @pl.when(i < BLOCKS)
        def _():
            transpose(i + BLOCKS)

    def pair(i, w, at_row, size):
        j, s = slots(i)
        return acc[s, rows(at_row, size, 32), :w] + r0[j, rows(at_row, size, 32), :w].astype(F32)

    def e_1(i, w):
        (j, s), (_, v) = slots(i), ring(i, 0)
        arrived(c0(i, w))
        p = lax.rem(v + 2, 4) * 256
        b1a[s, :, :w] = pair(i, w, p, 256).astype(BF)
        start(c1a(i, w))

    def e_2(i, w):
        (j, s), (_, v) = slots(i), ring(i, 0)
        arrived(c1a(i, w))
        for k, d in ((0, 1), (1, 3)):
            p, o = lax.rem(v + d, 4) * 256, 1 - k
            mine, other = (slice(FROM[x], FROM[x] + HALF[x]) for x in (k, o))
            b1b[s, k, mine, :w] = (pair(i, w, p + FROM[k], HALF[k]) + r1a[j, mine, :w].astype(F32)).astype(BF)
            b1b[s, k, other, :w] = pair(i, w, p + FROM[o], HALF[o]).astype(BF)
        start(c1b(i, w))

    def e_3(i, w):
        (j, s), (_, v), (_, x) = slots(i), ring(i, 0), ring(i, 1)
        sent(c1a(i, w))
        arrived(c1b(i, w))
        q2[s, :, :w] = pair(i, w, v * 256, 256) + r1b[j, 0, :, :w].astype(F32) + r1b[j, 1, :, :w].astype(F32)
        for k in range(3):
            b2[s, k, :, :w] = q2[s, rows(lax.rem(x + k + 1, 4) * 64, 64, 64), :w].astype(BF)
        start(c2(i, w))

    def e_4(i, w):
        (j, s), (_, x), (_, u) = slots(i), ring(i, 1), ring(i, 2)
        sent(c1b(i, w))
        arrived(c2(i, w))
        partial = q2[s, rows(x * 64, 64, 64), :w] + r2[j, 0, :, :w].astype(F32) + r2[j, 1, :, :w].astype(F32) + r2[j, 2, :, :w].astype(F32)
        r3[j, u, :, :w] = partial.astype(BF)
        start(c3(i, w))

    def e_5(i, w):
        (j, s), (_, v), (_, x) = slots(i), ring(i, 0), ring(i, 1)
        sent(c2(i, w))
        arrived(c3(i, w))
        total = r3[j, 0, :, :w].astype(F32) + r3[j, 1, :, :w].astype(F32) + r3[j, 2, :, :w].astype(F32) + r3[j, 3, :, :w].astype(F32)
        out[sums(i, 256 * v + 64 * x, 64, w)] = total.astype(BF)
        start(f2(i, w))

    def e_6(i, w):
        sent(c3(i, w))
        arrived(f2(i, w))
        start(f1a(i, w))
        start(f0(i, w, (0,)))

    def e_7(i, w):
        sent(f2(i, w))
        arrived(f1a(i, w))
        start(f1b(i, w))
        start(f0(i, w, (1, 2)))

    def e_8(i, w):
        sent(f1a(i, w))
        arrived(f1b(i, w))
        start(f0(i, w, (3,)))

    def e_9(i, w):
        sent(f1b(i, w))
        sent(f0(i, w, (0, 1, 2, 3)))

    owned = (e_1, e_2, e_3, e_4, e_5, e_6, e_7, e_8, e_9)

    def iteration(t, carry):
        @pl.when(t < NT)
        def _():
            e_0(t, owner(t) == c)

        for lag, step in zip(LAG[1:], owned):
            i = t - lag
            for w, fits in ((W, (i >= 0) & (i < WHOLE)), (128, (i >= WHOLE) & (i < NT))):
                @pl.when(fits & (owner(i) == c))
                def _(i=i, w=w, step=step):
                    step(i, w)

                if step is e_2 or step is e_9:
                    @pl.when(fits & (owner(i) != c))
                    def _(i=i, w=w, step=step):
                        if step is e_2:
                            sent(c0(i, w))
                        else:
                            arrived(f0(i, w, (0, 1, 2, 3)))

        return carry

    lax.fori_loop(0, NT + LAG[-1], iteration, 0)


def store(x, out, sems):
    copies = [pltpu.make_async_copy(x.at[i], out.at[i // PER, :, pl.ds(i % PER * W, W)], sems.at[i]) for i in range(WHOLE)]
    copies += [pltpu.make_async_copy(x.at[WHOLE, :, pl.ds(128 * n, 128)], out.at[n, :, pl.ds(PER * W, 128)], sems.at[WHOLE + n])
               for n in range(N)]
    for y in copies:
        y.start()
    for y in copies:
        y.wait()


def solution(mesh):
    dma = pltpu.SemaphoreType.DMA

    def step(a, g):
        sums = pl.pallas_call(
            kernel,
            out_shape=pltpu.VMEM((WHOLE + 1, D, W), BF),
            in_specs=[pl.BlockSpec(memory_space=pl.ANY)] * 2,
            out_specs=pl.BlockSpec(memory_space=pltpu.VMEM),
            scratch_shapes=[
                pltpu.VMEM((NA, CH, D), BF), pltpu.VMEM((N, D, T), BF), pltpu.VMEM((2, T, W), BF),
                pltpu.VMEM((R, D, W), F32), pltpu.VMEM((R, 256, W), F32),
                pltpu.VMEM((R, D, W), BF), pltpu.VMEM((R, 256, W), BF), pltpu.VMEM((R, 2, 256, W), BF),
                pltpu.VMEM((R, 3, 64, W), BF),
                pltpu.VMEM((OWN, D, W), BF), pltpu.VMEM((OWN, 256, W), BF), pltpu.VMEM((OWN, 2, 256, W), BF),
                pltpu.VMEM((OWN, 3, 64, W), BF), pltpu.VMEM((OWN, 4, 64, W), BF),
                dma((NA,)), dma((2,)),
                dma((R,)), dma((R, 2)), dma((R, 2)), dma((R, 3)), dma((R, 3)),
                dma((R, 3)), dma((R, 2)), dma((R, 2)), dma((R, 4)),
                dma((OWN,)), dma((OWN, 2)), dma((OWN, 2)), dma((OWN, 3)), dma((OWN, 3)),
                dma((OWN, 3)), dma((OWN, 2)), dma((OWN, 2)), dma((NT, 4)),
            ],
            compiler_params=pltpu.CompilerParams(collective_id=0, has_side_effects=True, vmem_limit_bytes=50 * 1024 * 1024),
        )(a, g)
        return pl.pallas_call(
            store,
            out_shape=jax.ShapeDtypeStruct((N, D, FF), BF),
            in_specs=[pl.BlockSpec(memory_space=pltpu.VMEM)],
            out_specs=pl.BlockSpec(memory_space=pl.ANY),
            scratch_shapes=[dma((NT,))],
            compiler_params=pltpu.CompilerParams(vmem_limit_bytes=1024 * 1024),
        )(sums)

    return jax.shard_map(step, mesh=mesh, in_specs=(P(("rep", "dp")), P(("rep", "dp"))), out_specs=P("rep"), check_vma=False)
```

```python
import jax
import jax.numpy as jnp
from jax import lax
from jax.experimental import pallas as pl
from jax.experimental.pallas import tpu as pltpu
from jax.sharding import PartitionSpec as P

BF, F32 = jnp.bfloat16, jnp.float32
MESH = pl.DeviceIdType.MESH
N, T, D, FF = 2, 4096, 1024, 3200
W = 256
PER = FF // W
WHOLE = N * PER
NT = WHOLE + N
OWN = NT // 2 + 1
R = 4
LAG = (0, 1, 3, 6, 8, 10, 13, 16, 18, 19)
HALF = (128, 128)
FROM = (0, HALF[0])
CH = 512
BLOCKS = T // CH
NA = 4


def rem(x, y):
    return x % y if isinstance(x, int) else lax.rem(x, y)


def div(x, y):
    return x // y if isinstance(x, int) else lax.div(x, y)


def pick(which, x, y):
    return (x if which else y) if isinstance(which, bool) else jnp.where(which, x, y)


def rows(start, size, unit):
    return pl.ds(start if isinstance(start, int) else pl.multiple_of(start, unit), size)


def kernel(a_ref, g_ref, out, raw, at, gb, acc, q2, b0, b1a, b1b, b2, r0, r1a, r1b, r2, r3,
           sem_a, sem_g, s0, s1a, s1b, s2, s3, t2, t1a, t1b, t0, d0, d1a, d1b, d2, d3, e2, e1a, e1b, e0):
    me = lax.axis_index("dp")
    c = rem(me, 2)
    mate = me + 1 - 2 * c

    def owner(i):
        return pick(i >= NT - 3, 1, pick(i == NT - 4, 0, 1 - rem(i, 2)))

    place = (div(me, 32), rem(div(me, 8), 4), rem(div(me, 2), 4))

    def ring(i, stage):
        axis = rem(i + stage, 3)
        return pick(axis == 0, 32, pick(axis == 1, 8, 2)), pick(axis == 0, place[0], pick(axis == 1, place[1], place[2]))

    def peer(r, d):
        stride, v = r
        return me + (rem(v + d, 4) - v) * stride

    def send(src, dst, send_sem, recv_sem, to):
        return pltpu.make_async_remote_copy(src_ref=src, dst_ref=dst, send_sem=send_sem, recv_sem=recv_sem,
                                            device_id={"dp": to}, device_id_type=MESH)

    def slots(i):
        j = pick(i == NT - 1, OWN - 1, div(i, 2))
        return j, rem(j, R)

    def c0(i, w):
        j, s = slots(i)
        return [send(b0.at[s, :, pl.ds(0, w)], r0.at[j, :, pl.ds(0, w)], s0.at[s], d0.at[j], mate)]

    def c1a(i, w):
        (j, s), r = slots(i), ring(i, 0)
        return [send(b1a.at[s, pl.ds(FROM[k], HALF[k]), pl.ds(0, w)], r1a.at[j, pl.ds(FROM[k], HALF[k]), pl.ds(0, w)], s1a.at[s, k], d1a.at[j, k], peer(r, d))
                for k, d in ((0, 1), (1, 3))]

    def c1b(i, w):
        (j, s), r = slots(i), ring(i, 0)
        return [send(b1b.at[s, k, :, pl.ds(0, w)], r1b.at[j, k, :, pl.ds(0, w)], s1b.at[s, k], d1b.at[j, k], peer(r, d)) for k, d in ((0, 1), (1, 3))]

    def c2(i, w):
        (j, s), r = slots(i), ring(i, 1)
        return [send(b2.at[s, k, :, pl.ds(0, w)], r2.at[j, k, :, pl.ds(0, w)], s2.at[s, k], d2.at[j, k], peer(r, k + 1)) for k in range(3)]

    def c3(i, w):
        (j, s), r = slots(i), ring(i, 2)
        return [send(r3.at[j, r[1], :, pl.ds(0, w)], r3.at[j, r[1], :, pl.ds(0, w)], s3.at[s, k], d3.at[j, k], peer(r, k + 1)) for k in range(3)]

    def sums(i, start, size, w):
        if w == W:
            return i, rows(start, size, 32), pl.ds(0, W)
        return WHOLE, rows(start, size, 32), rows(128 * (i - WHOLE), w, 128)

    def gather(i, w, start, size, to, ss, rs):
        piece = out.at[sums(i, start, size, w)]
        return send(piece, piece, ss, rs, to)

    def f2(i, w):
        (j, s), x1, x2 = slots(i), ring(i, 0), ring(i, 1)
        return [gather(i, w, 256 * x1[1] + 64 * x2[1], 64, peer(x2, k + 1), t2.at[s, k], e2.at[j, k]) for k in range(3)]

    def f1a(i, w):
        (j, s), x1 = slots(i), ring(i, 0)
        return [gather(i, w, 256 * x1[1], 256, peer(x1, d), t1a.at[s, k], e1a.at[j, k]) for k, d in ((0, 1), (1, 3))]

    def f1b(i, w):
        (j, s), x1 = slots(i), ring(i, 0)
        return [gather(i, w, 256 * rem(x1[1] + 4 - d, 4) + FROM[k], HALF[k], peer(x1, d), t1b.at[s, k], e1b.at[j, k])
                for k, d in ((0, 1), (1, 3))]

    def f0(i, w, which):
        (j, s), x1 = slots(i), ring(i, 0)
        return [gather(i, w, 256 * rem(x1[1] + d, 4), 256, mate, t0.at[s, k], e0.at[i, k])
                for k, d in ((0, 0), (1, 3), (2, 1), (3, 2)) if k in which]

    def start(copies):
        for x in copies:
            x.start()

    def arrived(copies):
        for x in copies:
            x.wait_recv()

    def sent(copies):
        for x in copies:
            x.wait_send()

    def gcopy(i):
        s = rem(i, 2)
        n, j = div(i, PER), rem(i, PER)
        return pltpu.make_async_copy(g_ref.at[0, n, :, pl.ds(pl.multiple_of(j * W, W), W)], gb.at[s], sem_g.at[s])

    def gnarrow(i):
        s = rem(i, 2)
        return pltpu.make_async_copy(g_ref.at[0, i - WHOLE, :, pl.ds(PER * W, 128)], gb.at[s, :, pl.ds(0, 128)], sem_g.at[s])

    def acopy(k):
        s = rem(k, NA)
        n, j = div(k, BLOCKS), rem(k, BLOCKS)
        return pltpu.make_async_copy(a_ref.at[0, n, rows(j * CH, CH, CH)], raw.at[s], sem_a.at[s])

    barrier = pltpu.get_barrier_semaphore()
    pl.semaphore_signal(barrier, inc=1, device_id={"dp": mate}, device_id_type=MESH)
    for axis in range(3):
        for d in (1, 2, 3):
            pl.semaphore_signal(barrier, inc=1, device_id={"dp": peer(ring(axis, 0), d)}, device_id_type=MESH)

    for k in range(NA - 1):
        acopy(k).start()
    gcopy(0).start()

    def transpose(k):
        @pl.when(k + NA - 1 < N * BLOCKS)
        def _():
            acopy(k + NA - 1).start()

        acopy(k).wait()
        n, j = div(k, BLOCKS), rem(k, BLOCKS)
        at[n, :, rows(j * CH, CH, CH)] = raw[rem(k, NA)].T

    def first(k, carry):
        transpose(k)
        return carry

    lax.fori_loop(0, BLOCKS, first, 0)
    pl.semaphore_wait(barrier, 10)

    def tile(i, w, mine):
        _, s = slots(i)
        r = jnp.dot(at[div(i, PER) if w == W else i - WHOLE], gb[rem(i, 2), :, :w], preferred_element_type=F32)
        if mine:
            acc[s, :, :w] = r
        else:
            b0[s, :, :w] = r.astype(BF)
            start(c0(i, w))

    def e_0(i, mine):
        @pl.when(i + 1 < WHOLE)
        def _():
            gcopy(i + 1).start()

        @pl.when((i + 1 >= WHOLE) & (i + 1 < NT))
        def _():
            gnarrow(i + 1).start()

        @pl.when(i < WHOLE)
        def _():
            gcopy(i).wait()

        @pl.when(i >= WHOLE)
        def _():
            gnarrow(i).wait()

        for w, fits in ((W, i < WHOLE), (128, i >= WHOLE)):
            @pl.when(fits & mine)
            def _(w=w):
                tile(i, w, True)

            @pl.when(fits & jnp.logical_not(mine))
            def _(w=w):
                tile(i, w, False)

        @pl.when(i < BLOCKS)
        def _():
            transpose(i + BLOCKS)

    def pair(i, w, at_row, size):
        j, s = slots(i)
        return acc[s, rows(at_row, size, 32), :w] + r0[j, rows(at_row, size, 32), :w].astype(F32)

    def e_1(i, w):
        (j, s), (_, v) = slots(i), ring(i, 0)
        arrived(c0(i, w))
        p = rem(v + 2, 4) * 256
        b1a[s, :, :w] = pair(i, w, p, 256).astype(BF)
        start(c1a(i, w))

    def e_2(i, w):
        (j, s), (_, v) = slots(i), ring(i, 0)
        arrived(c1a(i, w))
        for k, d in ((0, 1), (1, 3)):
            p, o = rem(v + d, 4) * 256, 1 - k
            mine, other = (slice(FROM[x], FROM[x] + HALF[x]) for x in (k, o))
            b1b[s, k, mine, :w] = (pair(i, w, p + FROM[k], HALF[k]) + r1a[j, mine, :w].astype(F32)).astype(BF)
            b1b[s, k, other, :w] = pair(i, w, p + FROM[o], HALF[o]).astype(BF)
        start(c1b(i, w))

    def e_3(i, w):
        (j, s), (_, v), (_, x) = slots(i), ring(i, 0), ring(i, 1)
        sent(c1a(i, w))
        arrived(c1b(i, w))
        q2[s, :, :w] = pair(i, w, v * 256, 256) + r1b[j, 0, :, :w].astype(F32) + r1b[j, 1, :, :w].astype(F32)
        for k in range(3):
            b2[s, k, :, :w] = q2[s, rows(rem(x + k + 1, 4) * 64, 64, 64), :w].astype(BF)
        start(c2(i, w))

    def e_4(i, w):
        (j, s), (_, x), (_, u) = slots(i), ring(i, 1), ring(i, 2)
        sent(c1b(i, w))
        arrived(c2(i, w))
        partial = q2[s, rows(x * 64, 64, 64), :w] + r2[j, 0, :, :w].astype(F32) + r2[j, 1, :, :w].astype(F32) + r2[j, 2, :, :w].astype(F32)
        r3[j, u, :, :w] = partial.astype(BF)
        start(c3(i, w))

    def e_5(i, w):
        (j, s), (_, v), (_, x) = slots(i), ring(i, 0), ring(i, 1)
        sent(c2(i, w))
        arrived(c3(i, w))
        total = r3[j, 0, :, :w].astype(F32) + r3[j, 1, :, :w].astype(F32) + r3[j, 2, :, :w].astype(F32) + r3[j, 3, :, :w].astype(F32)
        out[sums(i, 256 * v + 64 * x, 64, w)] = total.astype(BF)
        start(f2(i, w))

    def e_6(i, w):
        sent(c3(i, w))
        arrived(f2(i, w))
        start(f1a(i, w))
        start(f0(i, w, (0,)))

    def e_7(i, w):
        sent(f2(i, w))
        arrived(f1a(i, w))
        start(f1b(i, w))
        start(f0(i, w, (1, 2)))

    def e_8(i, w):
        sent(f1a(i, w))
        arrived(f1b(i, w))
        start(f0(i, w, (3,)))

    def e_9(i, w):
        sent(f1b(i, w))
        sent(f0(i, w, (0, 1, 2, 3)))

    owned = (e_1, e_2, e_3, e_4, e_5, e_6, e_7, e_8, e_9)

    def iteration(t, carry):
        e_0(t, owner(t) == c)
        for lag, step in zip(LAG[1:], owned):
            i = t - lag
            inside = (i >= 0) & (i < WHOLE)

            @pl.when(inside & (owner(i) == c))
            def _(i=i, step=step):
                step(i, W)

            if step is e_2 or step is e_9:
                @pl.when(inside & (owner(i) != c))
                def _(i=i, step=step):
                    other(i, W, step)

        return carry

    def other(i, w, step):
        if step is e_2:
            sent(c0(i, w))
        elif step is e_9:
            arrived(f0(i, w, (0, 1, 2, 3)))

    lax.fori_loop(0, NT, iteration, 0)

    for t in range(NT - 1, NT + LAG[-1]):
        left = [(t - lag, step) for lag, step in zip(LAG[1:], owned) if t - lag < NT and (t >= NT or t - lag >= WHOLE)]
        for core in (0, 1):
            @pl.when(c == core)
            def _(core=core, left=left):
                for i, step in left:
                    w = W if i < WHOLE else 128
                    if owner(i) == core:
                        step(i, w)
                    else:
                        other(i, w, step)


def store(x, out, sems):
    copies = [pltpu.make_async_copy(x.at[i], out.at[i // PER, :, pl.ds(i % PER * W, W)], sems.at[i]) for i in range(WHOLE)]
    copies += [pltpu.make_async_copy(x.at[WHOLE, :, pl.ds(128 * n, 128)], out.at[n, :, pl.ds(PER * W, 128)], sems.at[WHOLE + n])
               for n in range(N)]
    for y in copies:
        y.start()
    for y in copies:
        y.wait()


def solution(mesh):
    dma = pltpu.SemaphoreType.DMA

    def step(a, g):
        sums = pl.pallas_call(
            kernel,
            out_shape=pltpu.VMEM((WHOLE + 1, D, W), BF),
            in_specs=[pl.BlockSpec(memory_space=pl.ANY)] * 2,
            out_specs=pl.BlockSpec(memory_space=pltpu.VMEM),
            scratch_shapes=[
                pltpu.VMEM((NA, CH, D), BF), pltpu.VMEM((N, D, T), BF), pltpu.VMEM((2, T, W), BF),
                pltpu.VMEM((R, D, W), F32), pltpu.VMEM((R, 256, W), F32),
                pltpu.VMEM((R, D, W), BF), pltpu.VMEM((R, 256, W), BF), pltpu.VMEM((R, 2, 256, W), BF),
                pltpu.VMEM((R, 3, 64, W), BF),
                pltpu.VMEM((OWN, D, W), BF), pltpu.VMEM((OWN, 256, W), BF), pltpu.VMEM((OWN, 2, 256, W), BF),
                pltpu.VMEM((OWN, 3, 64, W), BF), pltpu.VMEM((OWN, 4, 64, W), BF),
                dma((NA,)), dma((2,)),
                dma((R,)), dma((R, 2)), dma((R, 2)), dma((R, 3)), dma((R, 3)),
                dma((R, 3)), dma((R, 2)), dma((R, 2)), dma((R, 4)),
                dma((OWN,)), dma((OWN, 2)), dma((OWN, 2)), dma((OWN, 3)), dma((OWN, 3)),
                dma((OWN, 3)), dma((OWN, 2)), dma((OWN, 2)), dma((NT, 4)),
            ],
            compiler_params=pltpu.CompilerParams(collective_id=0, has_side_effects=True, vmem_limit_bytes=50 * 1024 * 1024),
        )(a, g)
        return pl.pallas_call(
            store,
            out_shape=jax.ShapeDtypeStruct((N, D, FF), BF),
            in_specs=[pl.BlockSpec(memory_space=pltpu.VMEM)],
            out_specs=pl.BlockSpec(memory_space=pl.ANY),
            scratch_shapes=[dma((NT,))],
            compiler_params=pltpu.CompilerParams(vmem_limit_bytes=1024 * 1024),
        )(sums)

    return jax.shard_map(step, mesh=mesh, in_specs=(P(("rep", "dp")), P(("rep", "dp"))), out_specs=P("rep"), check_vma=False)
```
